32 devices in a mesh: blk: 8 (over z, y), tp: 4 (over x, core).
Axes of the slice: x: 2, y: 2, z: 4, core: 2. Of those that a mesh axis runs over, the one named last changes fastest.
Arguments:
- tokens: bfloat16 [2048, 2048], P('blk'), may hold values from -27 to 27
- order: int32 [16], replicated, may hold values from 0 to 15, each once
- gain_attn: float32 [2048], replicated, may hold values from 0.1 to 1.9
- gain_ffn: float32 [2048], replicated, may hold values from 0.1 to 1.9
- w_query: bfloat16 [2048, 2048], P(None, 'tp'), may hold values from -3.7565048 to 3.7565048
- w_key: bfloat16 [2048, 512], P(None, 'tp'), may hold values from -0.13258252 to 0.13258252
- w_value: bfloat16 [2048, 512], P(None, 'tp'), may hold values from -0.125 to 0.125
- w_out: bfloat16 [2048, 2048], P('tp'), may hold values from -0.125 to 0.125
- w_gate: bfloat16 [2048, 8192], P(None, 'tp'), may hold values from -0.125 to 0.125
- w_up: bfloat16 [2048, 8192], P(None, 'tp'), may hold values from -0.125 to 0.125
- w_down: bfloat16 [8192, 2048], P('tp'), may hold values from -0.0625 to 0.0625
Outputs:
- layer_out: bfloat16 [2048, 2048], P('blk', 'tp')
The draws below stay inside these ranges and needn't reach their ends.
Inputs may be any that keep to these rules, and one draw needn't show every extreme that they name: `order`: every number 0 to 15 appears once; device b of blk holds stored blocks 2b and 2b + 1.
All inputs are finite; a program needn't handle non-finite values.
Results may differ from the reference program's by a relative error of at most 0.0095.
Values may be sent and summed in bfloat16 or wider, within the bound.
A program may use at most 128 MiB of HBM per device.

```python
import math
import jax
import jax.numpy as jnp
from jax import lax

D = 2048
QH = 32
KVH = 8
HD = 64
FF = 8192
TOK_DEV = 256
SEQ = 2048
NCHUNK = 16
N_TP = 4


def shared_key_weight(key):
    base = jax.random.normal(jax.random.fold_in(key, 11), (D, KVH * HD), jnp.float32)
    return jnp.clip(base, -6.0, 6.0) * D ** (-0.5)


def draw_w_key(key, part):
    return shared_key_weight(key).astype(jnp.bfloat16)


def draw_w_query(key, part):
    noise = jax.random.normal(jax.random.fold_in(key, 12), (D, QH * HD), jnp.float32)
    noise = jnp.clip(noise, -6.0, 6.0) * (3.0 * D ** (-0.5))
    return noise.astype(jnp.bfloat16)


def draw_tokens(key, part):
    column = jnp.arange(D, dtype=jnp.float32) / (D - 1.0)
    rough = jax.random.uniform(jax.random.fold_in(key, 21), (D,), jnp.float32, 0.7, 1.3)
    col_scale = 0.5 * 4.0 ** column * rough
    base = jnp.clip(jax.random.normal(jax.random.fold_in(key, 24), (SEQ, D), jnp.float32), -6.0, 6.0)
    result = base * col_scale[None, :]
    return result.astype(jnp.bfloat16)


def level_of(rng, extent, shards, smallest, largest):
    factor_of = 1.0
    for dim, shards_of in shards:
        draws = jax.random.uniform(jax.random.fold_in(jax.random.fold_in(rng, 6), dim), (shards_of,), jnp.float32, smallest / len(shards), largest / len(shards))
        factor_of = factor_of * jnp.repeat(jnp.exp(draws), extent[dim] // shards_of).reshape((-1,) + (1,) * (len(extent) - 1 - dim))
    return factor_of


def normal_values(stream_key, shape, deviation, most, pieces=(), held_as=jnp.bfloat16):
    values = jax.random.normal(stream_key, shape, jnp.float32) * deviation
    if len(pieces) > 0:
        values = level_of(stream_key, shape, pieces, -0.22, 0.18) * values
    return jnp.clip(values, min=-most, max=most).astype(held_as)


def setup_inputs(seed: int = 0) -> dict:
    streams_of = jax.random.split(jax.random.key(seed), 12)
    return {
        "tokens": draw_tokens(jax.random.fold_in(streams_of[11], 71), 0),
        "order": jax.random.permutation(streams_of[1], NCHUNK).astype(jnp.int32),
        "gain_attn": jnp.clip(1.0 + 0.18 * jax.random.normal(streams_of[2], (D,), jnp.float32), 0.1, 1.9),
        "gain_ffn": jnp.clip(1.0 + 0.18 * jax.random.normal(streams_of[3], (D,), jnp.float32), 0.1, 1.9),
        "w_query": draw_w_query(jax.random.fold_in(streams_of[11], 71), 0),
        "w_key": draw_w_key(jax.random.fold_in(streams_of[11], 71), 0),
        "w_value": normal_values(streams_of[6], (D, KVH * HD), D ** -0.5, 0.125, ((1, 4),)),
        "w_out": normal_values(streams_of[7], (QH * HD, D), (QH * HD) ** -0.5, 0.125, ((0, 4),)),
        "w_gate": normal_values(streams_of[8], (D, FF), D ** -0.5, 0.125, ((1, 4),)),
        "w_up": normal_values(streams_of[9], (D, FF), D ** -0.5, 0.125, ((1, 4),)),
        "w_down": normal_values(streams_of[10], (FF, D), FF ** -0.5, 0.0625, ((0, 4),)),
    }


EPS = 1e-05
ROPE_BASE = 500000.0
MASKED = -1e+30

def rotate(values, positions):
    half_dim = values.shape[-1] // 2
    freq = ROPE_BASE ** (-(jnp.arange(half_dim, dtype=jnp.float32) * 2.0 / values.shape[-1]))
    angle = positions.astype(jnp.float32)[:, None] * freq[None, :]
    cosine = jnp.cos(angle)[:, None, :]
    sine = jnp.sin(angle)[:, None, :]
    first = values[..., :half_dim]
    second = values[..., half_dim:]
    return jnp.concatenate([first * cosine - second * sine, second * cosine + first * sine], axis=-1)

def reference(tokens, order, gain_attn, gain_ffn, w_query, w_key, w_value, w_out, w_gate, w_up, w_down):
    seq_len = tokens.shape[0]
    half_rows = TOK_DEV // 2
    stored = jnp.arange(seq_len, dtype=jnp.int32)
    position = order[stored // half_rows].astype(jnp.int32) * half_rows + stored % half_rows
    tokens_wide = tokens.astype(jnp.float32)
    normed = (tokens_wide * lax.rsqrt(lax.optimization_barrier(jnp.mean(tokens_wide * tokens_wide, axis=-1, keepdims=True)) + EPS) * gain_attn).astype(jnp.bfloat16)
    queries = jnp.dot(normed, w_query, preferred_element_type=jnp.float32).reshape(seq_len, QH, HD)
    queries = rotate(queries, position).astype(jnp.bfloat16)
    keys = jnp.dot(normed, w_key, preferred_element_type=jnp.float32).reshape(seq_len, KVH, HD)
    keys = rotate(keys, position).astype(jnp.bfloat16)
    values = jnp.dot(normed, w_value, preferred_element_type=jnp.float32).astype(jnp.bfloat16).reshape(seq_len, KVH, HD)
    group = QH // KVH
    query_block = math.gcd(seq_len, 256)
    grouped = queries.reshape(seq_len // query_block, query_block, KVH, group, HD)
    key_wide = keys.astype(jnp.float32)
    value_wide = values.astype(jnp.float32)
    scale = HD ** (-0.5)

    def one_block(inputs):
        block_queries, block_pos = inputs
        scores = jnp.einsum('qkgd,skd->kgqs', block_queries.astype(jnp.float32), key_wide) * scale
        allowed = position[None, :] <= block_pos[:, None]
        scores = jnp.where(allowed, scores, MASKED)
        highest = lax.optimization_barrier(jnp.max(scores, axis=-1, keepdims=True))
        weights = jnp.where(allowed, jnp.exp(scores - highest), 0.0)
        denominator = lax.optimization_barrier(jnp.sum(weights, axis=-1))
        rounded = lax.optimization_barrier(weights.astype(jnp.bfloat16)).astype(jnp.float32)
        mixed = jnp.einsum('kgqs,skd->qkgd', rounded, value_wide)
        return (mixed / jnp.transpose(denominator, (2, 0, 1))[..., None]).astype(jnp.bfloat16)
    heads = lax.map(one_block, (grouped, position.reshape(-1, query_block)))
    heads = heads.reshape(seq_len, QH * HD)
    head_share = QH * HD // N_TP
    attention = jnp.zeros((seq_len, D), jnp.float32)
    for member in range(N_TP):
        lower = member * head_share
        partial_value = jnp.dot(heads[:, lower:lower + head_share], w_out[lower:lower + head_share], preferred_element_type=jnp.float32)
        attention = attention + lax.optimization_barrier(partial_value.astype(jnp.bfloat16)).astype(jnp.float32)
    residual = tokens_wide + attention
    normed_ffn = (residual * lax.rsqrt(lax.optimization_barrier(jnp.mean(residual * residual, axis=-1, keepdims=True)) + EPS) * gain_ffn).astype(jnp.bfloat16)
    gate = jnp.dot(normed_ffn, w_gate, preferred_element_type=jnp.float32)
    up_proj = jnp.dot(normed_ffn, w_up, preferred_element_type=jnp.float32)
    hidden = (jax.nn.silu(gate) * up_proj).astype(jnp.bfloat16)
    unit_share = FF // N_TP
    feed = jnp.zeros((seq_len, D), jnp.float32)
    for member in range(N_TP):
        lower = member * unit_share
        partial_value = jnp.dot(hidden[:, lower:lower + unit_share], w_down[lower:lower + unit_share], preferred_element_type=jnp.float32)
        feed = feed + lax.optimization_barrier(partial_value.astype(jnp.bfloat16)).astype(jnp.float32)
    return (residual + feed).astype(jnp.bfloat16)
```

```python
import functools

import jax
import jax.numpy as jnp
from jax import lax
from jax.experimental import pallas as pl
from jax.experimental.pallas import tpu as pltpu
from jax.sharding import PartitionSpec as P

HD = 64
EPS = 1e-05
ROPE_BASE = 500000.0
MASKED = -1e30
MESH = pl.DeviceIdType.MESH
CHUNKS = 2
BF = jnp.bfloat16
F32 = jnp.float32


def dot(a, b):
    return jnp.dot(a, b, preferred_element_type=F32)


def ring_place(index, n):
    z, y = index // 2, index % 2
    return y * (n - 1 - z) + (1 - y) * z


def ring_index(place, n):
    place = lax.rem(place + 2 * n, n)
    far = place // (n // 2)
    return far * (2 * (n - 1 - place) + 1) + (1 - far) * (2 * place)


def kernel(
    n,
    tokens, gain_attn, gain_ffn, cosine, sine, qpos, kpos,
    w_query, w_key, w_value, w_out, w_gate, w_up, w_down,
    out,
    wq, wkv, wo, wg, wu, wd,
    normed, q_v, kv, m_v, acc, heads, resid, hidden, fin,
    p_send, p_recv, cs_mine, cs_peer, xr_mine, xr_peer,
    rs_send, rs_recv, xs_send, xs_recv,
    wsem, ksend, krecv, asend, arecv,
):
    rows, width = tokens.shape
    n_heads = q_v.shape[0]
    group = n_heads // 2
    half = width // 2
    share = width // 4
    blk = lax.axis_index("blk")
    tp = lax.axis_index("tp")
    core = lax.rem(tp, 2)
    xx = tp // 2
    peer = xx * 2 + (1 - core)
    across = (1 - xx) * 2 + core
    place = ring_place(blk, n)
    right = ring_index(place + 1, n)
    left = ring_index(place - 1, n)

    def load(src, dst, k):
        return pltpu.make_async_copy(src, dst, wsem.at[k])

    first = [
        load(w_key, wkv.at[:, 0:128], 0),
        load(w_value, wkv.at[:, 128:256], 1),
        load(w_query, wq, 2),
    ]
    for c in first:
        c.start()
    barrier = pltpu.get_barrier_semaphore()
    for target in ({"blk": right}, {"blk": left}, {"tp": peer}, {"tp": across}):
        pl.semaphore_signal(barrier, inc=1, device_id=target, device_id_type=MESH)

    wide = tokens[...].astype(F32)
    scale = lax.rsqrt(jnp.mean(wide * wide, axis=-1, keepdims=True) + EPS)
    normed[...] = (wide * scale * gain_attn[...]).astype(BF)

    lane = lax.broadcasted_iota(jnp.int32, (rows, 128), 1)
    low = lane < 64
    rope_first = (lane % 64) < 32

    def rope(u):
        turned = jnp.where(rope_first, pltpu.roll(u, 96, 1), pltpu.roll(u, 32, 1))
        return u * cosine[...] + turned * sine[...]

    first[0].wait()
    first[1].wait()
    rest = []
    for g in range(group):
        for b in range(2):
            rest.append(
                load(
                    w_out.at[pl.ds((b * group + g) * HD, HD)],
                    wo.at[pl.ds((2 * g + b) * HD, HD)],
                    6 + 2 * g + b,
                )
            )
    rest_ffn = [load(w_gate, wg, 3), load(w_up, wu, 4), load(w_down, wd, 5)]
    for c in rest:
        c.start()
    for c in rest_ffn:
        c.start()
    kv_new = dot(normed[...], wkv[...])
    kv[blk, :, 0:128] = rope(kv_new[:, 0:128]).astype(BF)
    kv[blk, :, 128:256] = kv_new[:, 128:256].astype(BF)
    pl.semaphore_wait(barrier, 4)

    hop = n // 2
    hrow = rows // 2

    def ring_copy(direction, step, part):
        toward = right if direction == 0 else left
        owner = ring_index(place - (step - 1) if direction == 0 else place + (step - 1), n)
        ref = kv.at[owner, pl.ds(part * hrow, hrow)]
        k = (direction * hop + step - 1) * 2 + part
        return pltpu.make_async_remote_copy(
            src_ref=ref, dst_ref=ref,
            send_sem=ksend.at[k], recv_sem=krecv.at[k],
            device_id={"blk": toward}, device_id_type=MESH,
        )

    def arrival(direction, step, part):
        owner = ring_index(place - step if direction == 0 else place + step, n)
        ref = kv.at[owner, pl.ds(part * hrow, hrow)]
        k = (direction * hop + step - 1) * 2 + part
        return pltpu.make_async_remote_copy(
            src_ref=ref, dst_ref=ref,
            send_sem=ksend.at[k], recv_sem=krecv.at[k],
            device_id={"blk": right if direction == 0 else left}, device_id_type=MESH,
        )

    def used(direction, step, part):
        return step < hop or part == direction

    sent = []

    def send(direction, step, part):
        if step <= hop and used(direction, step, part):
            c = ring_copy(direction, step, part)
            c.start()
            sent.append(c)

    for part in range(2):
        for direction in range(2):
            send(direction, 1, part)

    first[2].wait()
    for i in range(n_heads // 2):
        u = rope(dot(normed[...], wq[:, i * 128:(i + 1) * 128])) * (HD ** -0.5)
        turned = pltpu.roll(u, 64, 1)
        for b in range(2):
            j = 2 * i + b
            upper = j // group
            picked = u if upper == b else turned
            keep = low if upper == 0 else jnp.logical_not(low)
            q_v[j] = jnp.where(keep, picked, 0.0).astype(BF)

    def attend(blocks, fresh):
        biases = [
            jnp.where(kpos[b] <= qpos[...], 0.0, MASKED).astype(F32) for b in blocks
        ]
        ones = jnp.ones((rows, 128), BF)

        for j in range(n_heads):
            upper = j // group
            parts = [
                lax.dot_general(
                    q_v[j], kv[b, :, 0:128], (((1,), (1,)), ((), ())),
                    preferred_element_type=F32,
                ) + bias
                for b, bias in zip(blocks, biases)
            ]
            top = functools.reduce(
                jnp.maximum, [jnp.max(s, axis=1, keepdims=True) for s in parts]
            )
            if fresh:
                newest = jnp.broadcast_to(top, (rows, 128))
            else:
                old = m_v[j]
                newest = jnp.maximum(old, top)
            both = jnp.concatenate([newest] * (rows // 128), axis=1)
            total = None
            for b, s in zip(blocks, parts):
                vals = kv[b, :, 128:256]
                aug = jnp.where(low, vals, ones) if upper == 0 else jnp.where(low, ones, vals)
                d = dot(jnp.exp(s - both).astype(BF), aug)
                total = d if total is None else total + d
            if fresh:
                acc[j] = total
            else:
                acc[j] = acc[j] * jnp.exp(old - newest) + total
            m_v[j] = newest

    attend([blk], True)
    for step in range(1, hop + 1):
        for part in range(2):
            for direction in range(2):
                if used(direction, step, part):
                    arrival(direction, step, part).wait_recv()
                    send(direction, step + 1, part)
        if step < hop:
            attend([ring_index(place - step, n), ring_index(place + step, n)], False)
        else:
            attend([ring_index(place + step, n)], False)

    for g in range(group):
        a, b = acc[g], acc[group + g]
        a = a / pltpu.roll(a, 64, 1)
        b = b / pltpu.roll(b, 64, 1)
        heads[:, g * 128:(g + 1) * 128] = jnp.where(low, a, b).astype(BF)
    for c in rest:
        c.wait()

    count = rows // CHUNKS
    mine = pl.multiple_of(core * half, half)
    theirs = pl.multiple_of((1 - core) * half, half)
    span = [pl.ds(c * count, count) for c in range(CHUNKS)]

    def move(src, dst, k, c, target):
        return pltpu.make_async_remote_copy(
            src_ref=src, dst_ref=dst,
            send_sem=asend.at[k * CHUNKS + c], recv_sem=arecv.at[k * CHUNKS + c],
            device_id={"tp": target}, device_id_type=MESH,
        )

    give = [move(p_send.at[s], p_recv.at[s], 0, c, peer) for c, s in enumerate(span)]
    cross = [move(cs_mine.at[s], xr_mine.at[s], 1, c, across) for c, s in enumerate(span)]
    share_cs = [move(cs_mine.at[s], cs_peer.at[s], 2, c, peer) for c, s in enumerate(span)]
    forward = [move(xr_mine.at[s], xr_peer.at[s], 3, c, peer) for c, s in enumerate(span)]
    down_far = [
        move(rs_send.at[0, s], rs_recv.at[0, s], 4, c, peer) for c, s in enumerate(span)
    ]
    down_near = [
        move(rs_send.at[1, s], rs_recv.at[1, s], 5, c, peer) for c, s in enumerate(span)
    ]
    down_cross = [move(xs_send.at[s], xs_recv.at[s], 6, c, across) for c, s in enumerate(span)]

    for c, s in enumerate(span):
        p_send[s] = dot(heads[s], wo[:, pl.ds(theirs, half)]).astype(BF)
        give[c].start()
    for c, s in enumerate(span):
        own = dot(heads[s], wo[:, pl.ds(mine, half)]).astype(BF).astype(F32)
        give[c].wait_recv()
        cs_mine[s] = (own + p_recv[s].astype(F32)).astype(BF)
        cross[c].start()
        share_cs[c].start()

    def quarter(x_of, core_of):
        return pl.ds(pl.multiple_of((x_of * 2 + core_of) * share, share), share)

    for c, s in enumerate(span):
        cross[c].wait_recv()
        forward[c].start()
        a = tokens[s, pl.ds(mine, half)].astype(F32) + (
            cs_mine[s].astype(F32) + xr_mine[s].astype(F32)
        )
        resid[s, pl.ds(mine, half)] = a
        share_cs[c].wait_recv()
        forward[c].wait_recv()
        b = tokens[s, pl.ds(theirs, half)].astype(F32) + (
            cs_peer[s].astype(F32) + xr_peer[s].astype(F32)
        )
        resid[s, pl.ds(theirs, half)] = b
        square = jnp.sum(a * a, axis=-1, keepdims=True) + jnp.sum(b * b, axis=-1, keepdims=True)
        factor = lax.rsqrt(square / width + EPS)
        normed[s] = (resid[s] * factor * gain_ffn[...]).astype(BF)
        if c == 0:
            rest_ffn[0].wait()
            rest_ffn[1].wait()

        tile = 512

        @pl.loop(0, hidden.shape[1] // tile)
        def _(t):
            cols = pl.ds(pl.multiple_of(t * tile, tile), tile)
            gate = dot(normed[s], wg[:, cols])
            up = dot(normed[s], wu[:, cols])
            hidden[s, cols] = (gate / (1.0 + jnp.exp(-gate)) * up).astype(BF)

        if c == 0:
            rest_ffn[2].wait()
        rs_send[0, s] = dot(hidden[s], wd[:, quarter(1 - xx, 1 - core)]).astype(BF)
        down_far[c].start()
        own = dot(hidden[s], wd[:, quarter(1 - xx, core)]).astype(BF).astype(F32)
        down_far[c].wait_recv()
        xs_send[s] = (own + rs_recv[0, s].astype(F32)).astype(BF)
        down_cross[c].start()
        rs_send[1, s] = dot(hidden[s], wd[:, quarter(xx, 1 - core)]).astype(BF)
        down_near[c].start()
        own = dot(hidden[s], wd[:, quarter(xx, core)]).astype(BF).astype(F32)
        down_near[c].wait_recv()
        fin[s] = resid[s, quarter(xx, core)] + (own + rs_recv[1, s].astype(F32))
    for c, s in enumerate(span):
        down_cross[c].wait_recv()
        out[s] = (fin[s] + xs_recv[s].astype(F32)).astype(BF)
    for c in sent:
        c.wait_send()
    for c in range(CHUNKS):
        for group_of in (give, cross, share_cs, forward, down_far, down_near, down_cross):
            group_of[c].wait_send()


def local(n, tokens, order, gain_attn, gain_ffn, w_query, w_key, w_value, w_out, w_gate, w_up, w_down):
    rows, width = tokens.shape
    half_rows = rows // 2
    inner = w_query.shape[1]
    n_heads = inner // HD
    ffn = w_gate.shape[1]
    count = n * rows
    positions = (order[:, None] * half_rows + jnp.arange(half_rows, dtype=jnp.int32)[None, :]).reshape(
        n, 1, rows
    )
    blk = lax.axis_index("blk")
    query_pos = lax.dynamic_slice_in_dim(positions, blk, 1, 0).reshape(rows, 1)
    lanes = jnp.arange(128, dtype=jnp.int32)
    freq = ROPE_BASE ** (-((lanes % 32).astype(F32) * 2.0 / HD))
    angle = query_pos.astype(F32) * freq[None, :]
    cosine = jnp.cos(angle)
    sine = jnp.sin(angle) * jnp.where((lanes % HD) < HD // 2, -1.0, 1.0)[None, :]
    vmem = pl.BlockSpec(memory_space=pltpu.VMEM)
    hbm = pl.BlockSpec(memory_space=pl.ANY)
    V = pltpu.VMEM
    hop = n // 2
    return pl.pallas_call(
        functools.partial(kernel, n),
        out_shape=jax.ShapeDtypeStruct((rows, width // 4), BF),
        in_specs=[vmem] * 7 + [hbm] * 7,
        out_specs=vmem,
        scratch_shapes=[
            V((width, inner), BF), V((width, 256), BF), V((inner, width), BF),
            V((width, ffn), BF), V((width, ffn), BF), V((ffn, width), BF),
            V((rows, width), BF), V((n_heads, rows, 128), BF), V((n, rows, 256), BF),
            V((n_heads, rows, 128), F32), V((n_heads, rows, 128), F32),
            V((rows, inner), BF), V((rows, width), F32), V((rows, ffn), BF),
            V((rows, width // 4), F32),
        ]
        + [V((rows, width // 2), BF)] * 6
        + [
            V((2, rows, width // 4), BF), V((2, rows, width // 4), BF),
            V((rows, width // 4), BF), V((rows, width // 4), BF),
            pltpu.SemaphoreType.DMA((6 + n_heads,)),
            pltpu.SemaphoreType.DMA((4 * hop,)), pltpu.SemaphoreType.DMA((4 * hop,)),
            pltpu.SemaphoreType.DMA((7 * CHUNKS,)), pltpu.SemaphoreType.DMA((7 * CHUNKS,)),
        ],
        compiler_params=pltpu.CompilerParams(
            collective_id=0, has_side_effects=True, vmem_limit_bytes=60 * 1024 * 1024
        ),
    )(
        tokens, gain_attn.reshape(1, width), gain_ffn.reshape(1, width), cosine, sine,
        query_pos, positions,
        w_query, w_key, w_value, w_out, w_gate, w_up, w_down,
    )


def solution(mesh):
    placed = (
        P("blk", None), P(), P(), P(),
        P(None, "tp"), P(None, "tp"), P(None, "tp"), P("tp", None),
        P(None, "tp"), P(None, "tp"), P("tp", None),
    )
    return jax.shard_map(
        functools.partial(local, mesh.shape["blk"]),
        mesh=mesh, in_specs=placed, out_specs=P("blk", "tp"), check_vma=False,
    )
```

```python
import functools

import jax
import jax.numpy as jnp
import numpy as np
from jax import lax
from jax.experimental import pallas as pl
from jax.experimental.pallas import tpu as pltpu
from jax.sharding import PartitionSpec as P

HD = 64
EPS = 1e-05
ROPE_BASE = 500000.0
MASKED = -1e30
MESH = pl.DeviceIdType.MESH
CHUNKS = 2
PARTS = 4
BF = jnp.bfloat16
F32 = jnp.float32


def dot(a, b):
    return jnp.dot(a, b, preferred_element_type=F32)


def ring_place(index, n):
    z, y = index // 2, index % 2
    return y * (n - 1 - z) + (1 - y) * z


def ring_index(place, n):
    place = lax.rem(place + 2 * n, n)
    far = place // (n // 2)
    return far * (2 * (n - 1 - place) + 1) + (1 - far) * (2 * place)


def kernel(
    n,
    order, tokens, gain_attn, gain_ffn, freq, base_cos, base_sin,
    w_query, w_key, w_value, w_out, w_gate, w_up, w_down,
    out,
    wq, wkv, wo, wg, wu, wd,
    normed, q_v, kv, m_v, acc, heads, resid, hidden, fin,
    p_send, p_recv, cs_mine, cs_peer, xr_mine, xr_peer,
    rs_send, rs_recv, xs_send, xs_recv,
    wsem, ksend, krecv, asend, arecv,
):
    rows, width = tokens.shape
    n_heads = q_v.shape[0]
    group = n_heads // 2
    half = width // 2
    share = width // 4
    blk = lax.axis_index("blk")
    tp = lax.axis_index("tp")
    core = lax.rem(tp, 2)
    xx = tp // 2
    peer = xx * 2 + (1 - core)
    across = (1 - xx) * 2 + core
    place = ring_place(blk, n)
    right = ring_index(place + 1, n)
    left = ring_index(place - 1, n)

    def load(src, dst, k):
        return pltpu.make_async_copy(src, dst, wsem.at[k])

    first = [
        load(w_key, wkv.at[:, 0:128], 0),
        load(w_value, wkv.at[:, 128:256], 1),
        load(w_query, wq, 2),
    ]
    for c in first:
        c.start()
    barrier = pltpu.get_barrier_semaphore()
    for target in ({"blk": right}, {"blk": left}, {"tp": peer}, {"tp": across}):
        pl.semaphore_signal(barrier, inc=1, device_id=target, device_id_type=MESH)

    wide = tokens[...].astype(F32)
    scale = lax.rsqrt(jnp.mean(wide * wide, axis=-1, keepdims=True) + EPS)
    normed[...] = (wide * scale * gain_attn[...]).astype(BF)

    lane = lax.broadcasted_iota(jnp.int32, (rows, 128), 1)
    low = lane < 64
    rope_first = (lane % 64) < 32

    turn_rows = rows // 2

    def place_of(b, shape, axis):
        at = lax.broadcasted_iota(jnp.int32, shape, axis)
        return jnp.where(
            at < turn_rows, order[2 * b] * turn_rows + at, (order[2 * b + 1] - 1) * turn_rows + at
        )

    qpos = place_of(blk, (rows, 1), 0)
    cos_parts, sin_parts = [], []
    for h in range(2):
        start = (order[2 * blk + h] * turn_rows).astype(F32) * freq[...]
        c0, s0 = jnp.cos(start), jnp.sin(start)
        cos_parts.append(c0 * base_cos[...] - s0 * base_sin[...])
        sin_parts.append(s0 * base_cos[...] + c0 * base_sin[...])
    cosine = jnp.concatenate(cos_parts, axis=0)
    sine = jnp.concatenate(sin_parts, axis=0)
    sine = jnp.where(rope_first, -sine, sine)

    def rope(u):
        turned = jnp.where(rope_first, pltpu.roll(u, 96, 1), pltpu.roll(u, 32, 1))
        return u * cosine + turned * sine

    first[0].wait()
    first[1].wait()
    rest = []
    for g in range(group):
        for b in range(2):
            rest.append(
                load(
                    w_out.at[pl.ds((b * group + g) * HD, HD)],
                    wo.at[pl.ds((2 * g + b) * HD, HD)],
                    6 + 2 * g + b,
                )
            )
    rest_ffn = [load(w_gate, wg, 3), load(w_up, wu, 4), load(w_down, wd, 5)]
    for c in rest:
        c.start()
    for c in rest_ffn:
        c.start()
    kv_new = dot(normed[...], wkv[...])
    kv[blk, :, 0:128] = rope(kv_new[:, 0:128]).astype(BF)
    kv[blk, :, 128:256] = kv_new[:, 128:256].astype(BF)
    pl.semaphore_wait(barrier, 4)

    hop = n // 2
    hrow = rows // PARTS

    def ring_copy(direction, step, part):
        toward = right if direction == 0 else left
        owner = ring_index(place - (step - 1) if direction == 0 else place + (step - 1), n)
        ref = kv.at[owner, pl.ds(part * hrow, hrow)]
        k = (direction * hop + step - 1) * PARTS + part
        return pltpu.make_async_remote_copy(
            src_ref=ref, dst_ref=ref,
            send_sem=ksend.at[k], recv_sem=krecv.at[k],
            device_id={"blk": toward}, device_id_type=MESH,
        )

    def arrival(direction, step, part):
        owner = ring_index(place - step if direction == 0 else place + step, n)
        ref = kv.at[owner, pl.ds(part * hrow, hrow)]
        k = (direction * hop + step - 1) * PARTS + part
        return pltpu.make_async_remote_copy(
            src_ref=ref, dst_ref=ref,
            send_sem=ksend.at[k], recv_sem=krecv.at[k],
            device_id={"blk": right if direction == 0 else left}, device_id_type=MESH,
        )

    def used(direction, step, part):
        return step < hop or part // (PARTS // 2) == direction

    sent = []

    def send(direction, step, part):
        if step <= hop and used(direction, step, part):
            c = ring_copy(direction, step, part)
            c.start()
            sent.append(c)

    for part in range(PARTS):
        for direction in range(2):
            send(direction, 1, part)

    first[2].wait()
    for i in range(n_heads // 2):
        u = rope(dot(normed[...], wq[:, i * 128:(i + 1) * 128])) * (HD ** -0.5)
        turned = pltpu.roll(u, 64, 1)
        for b in range(2):
            j = 2 * i + b
            upper = j // group
            picked = u if upper == b else turned
            keep = low if upper == 0 else jnp.logical_not(low)
            q_v[j] = jnp.where(keep, picked, 0.0).astype(BF)

    def pump(step, part):
        for direction in range(2):
            if step <= hop and used(direction, step, part):
                arrival(direction, step, part).wait_recv()
                send(direction, step + 1, part)

    def attend(blocks, fresh, later):
        biases = [
            jnp.where(place_of(b, (1, rows), 1) <= qpos, 0.0, MASKED).astype(F32) for b in blocks
        ]
        ones = jnp.ones((rows, 128), BF)

        for j in range(n_heads):
            upper = j // group
            parts = [
                lax.dot_general(
                    q_v[j], kv[b, :, 0:128], (((1,), (1,)), ((), ())),
                    preferred_element_type=F32,
                ) + bias
                for b, bias in zip(blocks, biases)
            ]
            top = functools.reduce(
                jnp.maximum, [jnp.max(s, axis=1, keepdims=True) for s in parts]
            )
            if fresh:
                newest = jnp.broadcast_to(top, (rows, 128))
            else:
                old = m_v[j]
                newest = jnp.maximum(old, top)
            both = jnp.concatenate([newest] * (rows // 128), axis=1)
            total = None
            for b, s in zip(blocks, parts):
                vals = kv[b, :, 128:256]
                aug = jnp.where(low, vals, ones) if upper == 0 else jnp.where(low, ones, vals)
                d = dot(jnp.exp(s - both).astype(BF), aug)
                total = d if total is None else total + d
            if fresh:
                acc[j] = total
            else:
                acc[j] = acc[j] * jnp.exp(old - newest) + total
            m_v[j] = newest
            if (j + 1) % (n_heads // PARTS) == 0:
                pump(later, (j + 1) // (n_heads // PARTS) - 1)

    attend([blk], True, 1)
    for step in range(1, hop):
        attend([ring_index(place - step, n), ring_index(place + step, n)], False, step + 1)
    attend([ring_index(place + hop, n)], False, hop + 1)

    for g in range(group):
        a, b = acc[g], acc[group + g]
        a = a / pltpu.roll(a, 64, 1)
        b = b / pltpu.roll(b, 64, 1)
        heads[:, g * 128:(g + 1) * 128] = jnp.where(low, a, b).astype(BF)
    for c in rest:
        c.wait()

    count = rows // CHUNKS
    mine = pl.multiple_of(core * half, half)
    theirs = pl.multiple_of((1 - core) * half, half)
    span = [pl.ds(c * count, count) for c in range(CHUNKS)]

    def move(src, dst, k, c, target):
        return pltpu.make_async_remote_copy(
            src_ref=src, dst_ref=dst,
            send_sem=asend.at[k * CHUNKS + c], recv_sem=arecv.at[k * CHUNKS + c],
            device_id={"tp": target}, device_id_type=MESH,
        )

    give = [move(p_send.at[s], p_recv.at[s], 0, c, peer) for c, s in enumerate(span)]
    cross = [move(cs_mine.at[s], xr_mine.at[s], 1, c, across) for c, s in enumerate(span)]
    share_cs = [move(cs_mine.at[s], cs_peer.at[s], 2, c, peer) for c, s in enumerate(span)]
    forward = [move(xr_mine.at[s], xr_peer.at[s], 3, c, peer) for c, s in enumerate(span)]
    down_far = [
        move(rs_send.at[0, s], rs_recv.at[0, s], 4, c, peer) for c, s in enumerate(span)
    ]
    down_near = [
        move(rs_send.at[1, s], rs_recv.at[1, s], 5, c, peer) for c, s in enumerate(span)
    ]
    down_cross = [move(xs_send.at[s], xs_recv.at[s], 6, c, across) for c, s in enumerate(span)]

    for c, s in enumerate(span):
        p_send[s] = dot(heads[s], wo[:, pl.ds(theirs, half)]).astype(BF)
        give[c].start()
    for c, s in enumerate(span):
        own = dot(heads[s], wo[:, pl.ds(mine, half)]).astype(BF).astype(F32)
        give[c].wait_recv()
        cs_mine[s] = (own + p_recv[s].astype(F32)).astype(BF)
        cross[c].start()
        share_cs[c].start()

    def quarter(x_of, core_of):
        return pl.ds(pl.multiple_of((x_of * 2 + core_of) * share, share), share)

    for c, s in enumerate(span):
        cross[c].wait_recv()
        forward[c].start()
        a = tokens[s, pl.ds(mine, half)].astype(F32) + (
            cs_mine[s].astype(F32) + xr_mine[s].astype(F32)
        )
        resid[s, pl.ds(mine, half)] = a
        share_cs[c].wait_recv()
        forward[c].wait_recv()
        b = tokens[s, pl.ds(theirs, half)].astype(F32) + (
            cs_peer[s].astype(F32) + xr_peer[s].astype(F32)
        )
        resid[s, pl.ds(theirs, half)] = b
        square = jnp.sum(a * a, axis=-1, keepdims=True) + jnp.sum(b * b, axis=-1, keepdims=True)
        factor = lax.rsqrt(square / width + EPS)
        normed[s] = (resid[s] * factor * gain_ffn[...]).astype(BF)
        if c == 0:
            rest_ffn[0].wait()
            rest_ffn[1].wait()

        tile = 512

        @pl.loop(0, hidden.shape[1] // tile)
        def _(t):
            cols = pl.ds(pl.multiple_of(t * tile, tile), tile)
            gate = dot(normed[s], wg[:, cols])
            up = dot(normed[s], wu[:, cols])
            hidden[s, cols] = (gate / (1.0 + jnp.exp(-gate)) * up).astype(BF)

        if c == 0:
            rest_ffn[2].wait()
        rs_send[0, s] = dot(hidden[s], wd[:, quarter(1 - xx, 1 - core)]).astype(BF)
        down_far[c].start()
        rs_send[1, s] = dot(hidden[s], wd[:, quarter(xx, 1 - core)]).astype(BF)
        down_near[c].start()
        own = dot(hidden[s], wd[:, quarter(1 - xx, core)]).astype(BF).astype(F32)
        down_far[c].wait_recv()
        xs_send[s] = (own + rs_recv[0, s].astype(F32)).astype(BF)
        down_cross[c].start()
        own = dot(hidden[s], wd[:, quarter(xx, core)]).astype(BF).astype(F32)
        down_near[c].wait_recv()
        fin[s] = resid[s, quarter(xx, core)] + (own + rs_recv[1, s].astype(F32))
    for c, s in enumerate(span):
        down_cross[c].wait_recv()
        out[s] = (fin[s] + xs_recv[s].astype(F32)).astype(BF)
    for c in sent:
        c.wait_send()
    for c in range(CHUNKS):
        for group_of in (give, cross, share_cs, forward, down_far, down_near, down_cross):
            group_of[c].wait_send()


def local(n, tokens, order, gain_attn, gain_ffn, w_query, w_key, w_value, w_out, w_gate, w_up, w_down):
    rows, width = tokens.shape
    half_rows = rows // 2
    inner = w_query.shape[1]
    n_heads = inner // HD
    ffn = w_gate.shape[1]
    count = n * rows
    lanes = np.arange(128)
    freq = (ROPE_BASE ** (-((lanes % 32) * 2.0 / HD))).astype(np.float32)
    base = np.arange(half_rows)[:, None] * freq[None, :].astype(np.float64)
    base_cos, base_sin = np.cos(base).astype(np.float32), np.sin(base).astype(np.float32)
    vmem = pl.BlockSpec(memory_space=pltpu.VMEM)
    hbm = pl.BlockSpec(memory_space=pl.ANY)
    V = pltpu.VMEM
    hop = n // 2
    return pl.pallas_call(
        functools.partial(kernel, n),
        out_shape=jax.ShapeDtypeStruct((rows, width // 4), BF),
        in_specs=[pl.BlockSpec(memory_space=pltpu.SMEM)] + [vmem] * 6 + [hbm] * 7,
        out_specs=vmem,
        scratch_shapes=[
            V((width, inner), BF), V((width, 256), BF), V((inner, width), BF),
            V((width, ffn), BF), V((width, ffn), BF), V((ffn, width), BF),
            V((rows, width), BF), V((n_heads, rows, 128), BF), V((n, rows, 256), BF),
            V((n_heads, rows, 128), F32), V((n_heads, rows, 128), F32),
            V((rows, inner), BF), V((rows, width), F32), V((rows, ffn), BF),
            V((rows, width // 4), F32),
        ]
        + [V((rows, width // 2), BF)] * 6
        + [
            V((2, rows, width // 4), BF), V((2, rows, width // 4), BF),
            V((rows, width // 4), BF), V((rows, width // 4), BF),
            pltpu.SemaphoreType.DMA((6 + n_heads,)),
            pltpu.SemaphoreType.DMA((2 * PARTS * hop,)), pltpu.SemaphoreType.DMA((2 * PARTS * hop,)),
            pltpu.SemaphoreType.DMA((7 * CHUNKS,)), pltpu.SemaphoreType.DMA((7 * CHUNKS,)),
        ],
        compiler_params=pltpu.CompilerParams(
            collective_id=0, has_side_effects=True, vmem_limit_bytes=60 * 1024 * 1024
        ),
    )(
        order, tokens, gain_attn.reshape(1, width), gain_ffn.reshape(1, width),
        jnp.asarray(freq[None, :]), jnp.asarray(base_cos), jnp.asarray(base_sin),
        w_query, w_key, w_value, w_out, w_gate, w_up, w_down,
    )


def solution(mesh):
    placed = (
        P("blk", None), P(), P(), P(),
        P(None, "tp"), P(None, "tp"), P(None, "tp"), P("tp", None),
        P(None, "tp"), P(None, "tp"), P("tp", None),
    )
    return jax.shard_map(
        functools.partial(local, mesh.shape["blk"]),
        mesh=mesh, in_specs=placed, out_specs=P("blk", "tp"), check_vma=False,
    )
```
